512 devices in a mesh: slab: 128 (over z_lo, y, x, core), det: 4 (over z_hi).
Axes of the slice: x: 4, y: 4, z: 16 (z_hi: 4, z_lo: 4; z = z_hi * 4 + z_lo), core: 2. Of those that a mesh axis runs over, the one named last changes fastest.
Arguments:
- traces: float32 [512, 128, 4096], P(('slab', 'det')), may hold values from -6 to 6
- tables: bfloat16 [512, 256, 2048], P('slab', None, 'det'), may hold values from -0.0625 to 0.0625
- slab_range: int32 [512, 2], P(('slab', 'det')), may hold values from 0 to 127, as said below
- table_slot: int32 [512, 7], P(('slab', 'det')), may hold values from 0 to 3
- sample_start: int32 [512, 7], P(('slab', 'det')), may hold values from 0 to 3840
Outputs:
- image: float32 [128, 262144], P(None, ('slab', 'det'))
The draws below stay inside these ranges and needn't reach their ends.
Inputs may be any that keep to these rules, and one draw needn't show every extreme that they name: For detector d with home slab g = d // 4: max(0, g - 3) <= slab_range[d, 0] <= g <= slab_range[d, 1] <= min(127, g + 3); some detectors reach the full 3 on both sides where the grid allows.
All inputs are finite; a program needn't handle non-finite values.
Results may differ from the reference program's by a relative error of at most 0.007.
Values may be sent and summed in bfloat16 or wider, within the bound.
A program may use at most 64 MiB of HBM per device.

```python
import jax
import jax.numpy as jnp
from jax import lax

SAMP = 4096
KWIN = 256
NTAB = 4
RANGE = 3
VOX = 2048
FRAMES = 128
DET_DEV = 1
DETS = 512
N_SLAB = 128
N_DET = 4


def draw_slab_range(key, part):
    lower_key, upper_key = jax.random.split(jax.random.fold_in(key, 11))
    detector_index = jnp.arange(DETS, dtype=jnp.int32)
    home = detector_index // (N_DET * DET_DEV)
    lower_reach = jax.random.randint(lower_key, (DETS,), 0, RANGE + 1)
    upper_reach = jax.random.randint(upper_key, (DETS,), 0, RANGE + 1)
    widest = detector_index % 7 == 0
    lower_reach = jnp.where(widest, RANGE, lower_reach)
    upper_reach = jnp.where(widest, RANGE, upper_reach)
    first_slab = jnp.maximum(home - lower_reach, 0)
    last_slab = jnp.minimum(home + upper_reach, N_SLAB - 1)
    return jnp.stack([first_slab, last_slab], axis=1).astype(jnp.int32)


def plant(entries, rng, smallest, largest):
    longest = entries.shape.index(max(entries.shape))
    spots = []
    for shift in (0, 1):
        where = [jax.random.randint(jax.random.fold_in(rng, axis), (), 0, length) for axis, length in enumerate(entries.shape)]
        where[longest] = (where[longest] + shift) % entries.shape[longest]
        spots.append(tuple(where))
    return entries.at[spots[0]].set(smallest).at[spots[1]].set(largest)


def block_levels(key, shape, cuts, smallest, top_value):
    def one(dim, parts):
        steps = jax.random.uniform(jax.random.fold_in(jax.random.fold_in(key, 6), dim), (parts,), jnp.float32, smallest / len(cuts), top_value / len(cuts))
        return jnp.repeat(jnp.exp(steps), shape[dim] // parts).reshape((-1,) + (1,) * (len(shape) - dim - 1))

    loudness = one(*cuts[0])
    for cut in cuts[1:]:
        loudness = loudness * one(*cut)
    return loudness


def normal_values(key, shape, deviation, bound, cuts=(), kind=jnp.bfloat16):
    array = jax.random.normal(key, shape, jnp.float32) * deviation
    if len(cuts) > 0:
        array = block_levels(key, shape, cuts, -0.22, 0.18) * array
    return jnp.clip(array, min=-bound, max=bound).astype(kind)


def setup_inputs(seed: int = 0) -> dict:
    splits = jax.random.split(jax.random.key(seed), 6)
    traces = normal_values(splits[0], (DETS, FRAMES, SAMP), 1.0, 6.0, ((0, 512),), jnp.float32)
    tables = normal_values(splits[1], (N_SLAB * NTAB, KWIN, N_SLAB * 0 + VOX), (4 * (2 * RANGE + 1) * DET_DEV * KWIN) ** -0.5, 0.0625, ((0, 128), (2, 4)))
    slab_range = draw_slab_range(jax.random.fold_in(splits[5], 71), 0)
    table_slot = plant(jax.random.randint(splits[3], (DETS, 2 * RANGE + 1), 0, NTAB), jax.random.fold_in(splits[3], 1), 0, NTAB - 1).astype(jnp.int32)
    sample_start = plant(jax.random.randint(splits[4], (DETS, 2 * RANGE + 1), 0, SAMP - KWIN + 1), jax.random.fold_in(splits[4], 1), 0, SAMP - KWIN).astype(jnp.int32)
    return {"traces": traces, "tables": tables, "slab_range": slab_range, "table_slot": table_slot, "sample_start": sample_start}


def windows_for(trace_rows, starts):
    def single(trace_row, first_index):
        return lax.dynamic_slice_in_dim(trace_row, first_index, KWIN, 1)
    return jax.vmap(single)(trace_rows, starts)


def reference(traces, tables, slab_range, table_slot, sample_start):
    group = N_DET * DET_DEV
    table_blocks = tables.reshape(N_SLAB, NTAB, KWIN, VOX)
    slot_values = jnp.arange(NTAB, dtype=jnp.int32)

    def one_slab(slab):
        stacked = jnp.zeros((N_DET, NTAB, FRAMES, KWIN), jnp.float32)
        for offset in range(-RANGE, RANGE + 1):
            home = slab - offset
            valid = (home >= 0) & (home < N_SLAB)
            clipped = jnp.clip(home, 0, N_SLAB - 1)
            first_row = (clipped * group).astype(jnp.int32)
            trace_rows = lax.dynamic_slice_in_dim(traces, first_row, group, 0).astype(jnp.bfloat16)
            ranges = lax.dynamic_slice_in_dim(slab_range, first_row, group, 0)
            slot_ids = lax.dynamic_slice_in_dim(table_slot, first_row, group, 0)[:, offset + RANGE]
            starts = lax.dynamic_slice_in_dim(sample_start, first_row, group, 0)[:, offset + RANGE]
            active = valid & (ranges[:, 0] <= slab) & (slab <= ranges[:, 1])
            windows = windows_for(trace_rows, starts).astype(jnp.float32)
            windows = windows.reshape(N_DET, DET_DEV, FRAMES, KWIN)
            onehot = ((slot_ids[:, None] == slot_values[None, :]) & active[:, None]).astype(jnp.float32)
            onehot = onehot.reshape(N_DET, DET_DEV, NTAB)
            stacked = stacked + jnp.einsum("kit,kifw->ktfw", onehot, windows)
        rounded = stacked.astype(jnp.bfloat16).astype(jnp.float32)
        weights = table_blocks[slab].astype(jnp.float32)
        return jnp.einsum("ktfw,twv->fv", rounded, weights)

    slabs = lax.map(one_slab, jnp.arange(N_SLAB, dtype=jnp.int32))
    return jnp.transpose(slabs, (1, 0, 2)).reshape(FRAMES, N_SLAB * VOX)
```

```python
import functools

import jax
import jax.numpy as jnp
from jax import lax
from jax.experimental import pallas as pl
from jax.experimental.pallas import tpu as pltpu
from jax.sharding import PartitionSpec as P

KWIN = 256
NTAB = 4
RANGE = 3
CHUNKS = 4
LANES = 128
MESH = pl.DeviceIdType.MESH
OFFSETS = [1, -1, 2, -2, 3, -3]


def kernel(
    n_slab, rows, span_ref, slot_ref, start_ref, traces_ref, tables_ref, out_ref,
    trace_v, moves, win, got, slots_out, slots_in, stack, part, full, land1, land2, land3, tab, out_v,
    load_sem, tab_sem, store_sem, slot_send, slot_recv, win_send, win_recv, z_send, z_recv,
):
    slab = lax.axis_index("slab")
    det = lax.axis_index("det")
    side = det + 1 - 2 * lax.rem(det, 2)
    across = 3 - det
    keep_a = lax.rem((det + 1) // 2, 2)
    keep_b = 2 + det // 2
    give_a = 1 - keep_a
    give_b = 5 - keep_b
    first = (side, across)
    second = (across, side)
    keeps = (keep_a, keep_b)
    gives = (give_a, give_b)

    def inside(s):
        return jnp.logical_and(s >= 0, s < n_slab)

    def piece(c):
        return pl.ds(c * rows, rows)

    n_tiles = trace_v.shape[0]

    @pl.loop(0, n_tiles)
    def _(tile):
        pltpu.make_async_copy(
            traces_ref.at[0, :, pl.ds(pl.multiple_of(tile * LANES, LANES), LANES)],
            trace_v.at[tile], load_sem,
        ).start()

    tab_load = pltpu.make_async_copy(tables_ref, tab, tab_sem)
    tab_load.start()

    barrier = pltpu.get_barrier_semaphore()
    friends = 2
    for peer in (side, across):
        pl.semaphore_signal(barrier, inc=1, device_id=(slab, peer), device_id_type=MESH)
    for o in OFFSETS:
        there = inside(slab + o)
        friends = friends + there.astype(jnp.int32)

        @pl.when(there)
        def _():
            pl.semaphore_signal(barrier, inc=1, device_id=(slab + o, det), device_id_type=MESH)

    flat = (8, LANES)
    low = jnp.full(flat, span_ref[0, 0], jnp.int32)
    high = jnp.full(flat, span_ref[0, 1], jnp.int32)
    for i in range(2 * RANGE + 1):
        target = slab + (i - RANGE)
        active = jnp.logical_and(low <= target, target <= high)
        slots_out[i] = jnp.where(active, jnp.full(flat, slot_ref[0, i], jnp.int32), -1)
    for o in OFFSETS:
        i = o + RANGE

        @pl.when(jnp.logical_not(inside(slab - o)))
        def _():
            slots_in[i] = jnp.full((8, LANES), -1, jnp.int32)
            got[i] = jnp.zeros((CHUNKS * rows, KWIN), jnp.bfloat16)

    down = lax.broadcasted_iota(jnp.int32, (2 * LANES, LANES), 0)
    along = lax.broadcasted_iota(jnp.int32, (2 * LANES, LANES), 1)
    for i in range(2 * RANGE + 1):
        shift = lax.rem(start_ref[0, i], LANES)
        moves[i] = jnp.where(down - along == shift, 1.0, 0.0).astype(jnp.bfloat16)

    def cut(i, c):
        tile = lax.div(start_ref[0, i], LANES)
        last = lax.min(tile + 2, n_tiles - 1)
        tiles = [trace_v[spot, piece(c), :].astype(jnp.bfloat16) for spot in (tile, tile + 1, last)]
        for h in range(2):
            pair = jnp.concatenate([tiles[h], tiles[h + 1]], axis=1)
            win[i, piece(c), pl.ds(h * LANES, LANES)] = jnp.dot(
                pair, moves[i], preferred_element_type=jnp.float32
            ).astype(jnp.bfloat16)

    def slot_copy(o):
        i = o + RANGE
        return pltpu.make_async_remote_copy(
            src_ref=slots_out.at[i], dst_ref=slots_in.at[i],
            send_sem=slot_send.at[i], recv_sem=slot_recv.at[i],
            device_id=(slab + o, det), device_id_type=MESH,
        )

    def win_copy(o, c):
        i = o + RANGE
        return pltpu.make_async_remote_copy(
            src_ref=win.at[i, piece(c), :], dst_ref=got.at[i, piece(c), :],
            send_sem=win_send.at[i, c], recv_sem=win_recv.at[i, c],
            device_id=(slab + o, det), device_id_type=MESH,
        )

    def z_copy(step, cls, c, src, dst, peer):
        return pltpu.make_async_remote_copy(
            src_ref=src, dst_ref=dst,
            send_sem=z_send.at[step, cls, c], recv_sem=z_recv.at[step, cls, c],
            device_id=(slab, peer), device_id_type=MESH,
        )

    def step1(cls, c):
        return z_copy(
            0, cls, c, stack.at[gives[cls], piece(c), :], land1.at[cls, piece(c), :], first[cls]
        )

    def step2(cls, c):
        return z_copy(
            1, cls, c, part.at[cls, piece(c), :], land2.at[cls, piece(c), :], second[cls]
        )

    def step3(cls, c):
        return z_copy(
            2, cls, c, full.at[cls, piece(c), :], land3.at[cls, piece(c), :], first[cls]
        )

    pltpu.make_async_copy(trace_v, trace_v, load_sem).wait()
    for c in range(CHUNKS):
        for i in range(2 * RANGE + 1):
            cut(i, c)
        if c == 0:
            pl.semaphore_wait(barrier, friends)
            for o in OFFSETS:

                @pl.when(inside(slab + o))
                def _():
                    slot_copy(o).start()

        for o in OFFSETS:

            @pl.when(inside(slab + o))
            def _():
                win_copy(o, c).start()

    for o in OFFSETS:

        @pl.when(inside(slab - o))
        def _():
            slot_copy(o).wait_recv()

    for c in range(CHUNKS):
        for o in OFFSETS:

            @pl.when(inside(slab - o))
            def _():
                win_copy(o, c).wait_recv()

        for h in range(2):
            cols = pl.ds(h * LANES, LANES)
            sums = [jnp.zeros((rows, LANES), jnp.float32) for _ in range(NTAB)]
            for o in [0, *OFFSETS]:
                i = o + RANGE
                source, slots = (win, slots_out) if o == 0 else (got, slots_in)
                window = source[i, piece(c), cols].astype(jnp.float32)
                block = jnp.broadcast_to(slots[i, 0:1, :], (rows, LANES))
                for t in range(NTAB):
                    sums[t] = sums[t] + jnp.where(block == t, window, 0.0)
            for t in range(NTAB):
                stack[t, piece(c), cols] = sums[t].astype(jnp.bfloat16)
        for cls in range(2):
            step1(cls, c).start()

    for c in range(CHUNKS):
        for cls in range(2):
            step1(cls, c).wait_recv()
            mine = stack[keeps[cls], piece(c), :].astype(jnp.float32)
            theirs = land1[cls, piece(c), :].astype(jnp.float32)
            part[cls, piece(c), :] = (mine + theirs).astype(jnp.bfloat16)
            step2(cls, c).start()

    for c in range(CHUNKS):
        for cls in range(2):
            step2(cls, c).wait_recv()
            mine = part[cls, piece(c), :].astype(jnp.float32)
            theirs = land2[cls, piece(c), :].astype(jnp.float32)
            full[cls, piece(c), :] = (mine + theirs).astype(jnp.bfloat16)
            step3(cls, c).start()

    tab_load.wait()
    out_v[...] = jnp.dot(
        full[0], tab[keeps[0]], preferred_element_type=jnp.float32
    ) + jnp.dot(full[1], tab[keeps[1]], preferred_element_type=jnp.float32)
    stores = []
    for c in range(CHUNKS):
        total = out_v[piece(c), :]
        for cls in range(2):
            step3(cls, c).wait_recv()
            total = total + jnp.dot(
                land3[cls, piece(c), :], tab[gives[cls]], preferred_element_type=jnp.float32
            )
        out_v[piece(c), :] = total
        store = pltpu.make_async_copy(
            out_v.at[piece(c), :], out_ref.at[piece(c), :], store_sem.at[c]
        )
        store.start()
        stores.append(store)

    for o in OFFSETS:

        @pl.when(inside(slab + o))
        def _():
            slot_copy(o).wait_send()
            for c in range(CHUNKS):
                win_copy(o, c).wait_send()

    for c in range(CHUNKS):
        for cls in range(2):
            step1(cls, c).wait_send()
            step2(cls, c).wait_send()
            step3(cls, c).wait_send()
        stores[c].wait()


def body(n_slab, traces, tables, slab_range, table_slot, sample_start):
    _, frames, samp = traces.shape
    vox = tables.shape[2]
    rows = frames // CHUNKS
    reach = 2 * RANGE + 1
    smem = pl.BlockSpec(memory_space=pltpu.SMEM)
    far = pl.BlockSpec(memory_space=pl.ANY)
    half = pltpu.VMEM((2, frames, KWIN), jnp.bfloat16)
    dma = pltpu.SemaphoreType.DMA
    return pl.pallas_call(
        functools.partial(kernel, n_slab, rows),
        out_shape=jax.ShapeDtypeStruct((frames, vox), jnp.float32),
        in_specs=[smem, smem, smem, far, far],
        out_specs=far,
        scratch_shapes=[
            pltpu.VMEM((samp // LANES, frames, LANES), jnp.float32),
            pltpu.VMEM((reach, 2 * LANES, LANES), jnp.bfloat16),
            pltpu.VMEM((reach, frames, KWIN), jnp.bfloat16),
            pltpu.VMEM((reach, frames, KWIN), jnp.bfloat16),
            pltpu.VMEM((reach, 8, LANES), jnp.int32),
            pltpu.VMEM((reach, 8, LANES), jnp.int32),
            pltpu.VMEM((NTAB, frames, KWIN), jnp.bfloat16),
            half, half, half, half, half,
            pltpu.VMEM((NTAB, KWIN, vox), jnp.bfloat16),
            pltpu.VMEM((frames, vox), jnp.float32),
            dma, dma, dma((CHUNKS,)),
            dma((reach,)), dma((reach,)),
            dma((reach, CHUNKS)), dma((reach, CHUNKS)),
            dma((3, 2, CHUNKS)), dma((3, 2, CHUNKS)),
        ],
        compiler_params=pltpu.CompilerParams(collective_id=0, has_side_effects=True),
    )(slab_range, table_slot, sample_start, traces, tables)


def solution(mesh):
    placed = (
        P(("slab", "det"), None, None),
        P("slab", None, "det"),
        P(("slab", "det"), None),
        P(("slab", "det"), None),
        P(("slab", "det"), None),
    )
    return jax.shard_map(
        functools.partial(body, mesh.shape["slab"]),
        mesh=mesh, in_specs=placed, out_specs=P(None, ("slab", "det")), check_vma=False,
    )
```

```python
import functools

import jax
import jax.numpy as jnp
from jax import lax
from jax.experimental import pallas as pl
from jax.experimental.pallas import tpu as pltpu
from jax.sharding import PartitionSpec as P

KWIN = 256
NTAB = 4
RANGE = 3
REACH = 2 * RANGE + 1
SIZES = (16, 16, 32, 32, 32)
CHUNKS = len(SIZES)
LANES = 128
MESH = pl.DeviceIdType.MESH
OFFSETS = [3, -3, 2, -2, 1, -1]


def kernel(
    n_slab, traces_ref, tables_ref, span_hbm, slot_hbm, start_hbm, out_ref,
    span_ref, slot_ref, start_ref, trace_v, moves, win, got, slots_out, slots_in,
    stack, sums, land, tab,
    int_sem, load_sem, tab_sem, slot_send, slot_recv, win_send, win_recv, z_send, z_recv, hello,
):
    slab = lax.axis_index("slab")
    det = lax.axis_index("det")
    side = det + 1 - 2 * lax.rem(det, 2)
    across = 3 - det
    keep_a = lax.rem((det + 1) // 2, 2)
    keep_b = 2 + det // 2
    first = (side, across)
    second = (across, side)
    keeps = (keep_a, keep_b)
    gives = (1 - keep_a, 5 - keep_b)
    n_tiles = trace_v.shape[0]
    near = jnp.minimum(slab, RANGE) + jnp.minimum(n_slab - 1 - slab, RANGE)

    def inside(s):
        return jnp.logical_and(s >= 0, s < n_slab)

    def piece(c):
        return pl.ds(sum(SIZES[:c]), SIZES[c])

    def wait_bytes(ref, sem):
        pltpu.make_async_copy(ref, ref, sem).wait()

    def wait_near(refs, sem):
        for n in range(RANGE, 2 * RANGE + 1):

            @pl.when(near == n)
            def _():
                wait_bytes(refs(n), sem)

    barrier = pltpu.get_barrier_semaphore()
    greets_side = jnp.logical_or(det == 0, det == 3)
    greets_across = det < 2
    friends = near + jnp.where(det == 2, 2, jnp.where(det == 0, 0, 1))

    @pl.when(greets_side)
    def _():
        pl.semaphore_signal(barrier, inc=1, device_id=(slab, side), device_id_type=MESH)

    @pl.when(greets_across)
    def _():
        pl.semaphore_signal(barrier, inc=1, device_id=(slab, across), device_id_type=MESH)

    for o in OFFSETS:

        @pl.when(inside(slab + o))
        def _():
            pl.semaphore_signal(barrier, inc=1, device_id=(slab + o, det), device_id_type=MESH)

    ints = [
        pltpu.make_async_copy(src, dst, int_sem.at[n])
        for n, (src, dst) in enumerate(
            [(start_hbm, start_ref), (span_hbm, span_ref), (slot_hbm, slot_ref)]
        )
    ]
    for copy in ints:
        copy.start()

    @pl.loop(0, n_tiles)
    def _(tile):
        pltpu.make_async_copy(
            traces_ref.at[0, :, pl.ds(pl.multiple_of(tile * LANES, LANES), LANES)],
            trace_v.at[tile], load_sem,
        ).start()

    tab_load = pltpu.make_async_copy(tables_ref, tab, tab_sem)

    for copy in ints:
        copy.wait()

    flat = (8, LANES)
    low = jnp.full(flat, span_ref[0, 0], jnp.int32)
    high = jnp.full(flat, span_ref[0, 1], jnp.int32)
    for q, o in enumerate([*OFFSETS, 0]):
        target = slab + o
        active = jnp.logical_and(low <= target, target <= high)
        slots_out[q] = jnp.where(active, jnp.full(flat, slot_ref[0, o + RANGE], jnp.int32), -1)
    for q, o in enumerate(OFFSETS):

        @pl.when(jnp.logical_not(inside(slab - o)))
        def _():
            slots_in[q] = jnp.full(flat, -1, jnp.int32)
            got[q] = jnp.zeros(got.shape[1:], jnp.bfloat16)

    down = lax.broadcasted_iota(jnp.int32, (2 * LANES, LANES), 0)
    along = lax.broadcasted_iota(jnp.int32, (2 * LANES, LANES), 1)
    for q, o in enumerate([*OFFSETS, 0]):
        shift = lax.rem(start_ref[0, o + RANGE], LANES)
        moves[q] = jnp.where(down - along == shift, 1.0, 0.0).astype(jnp.bfloat16)

    def cut(q, o, c):
        tile = lax.div(start_ref[0, o + RANGE], LANES)
        last = lax.min(tile + 2, n_tiles - 1)
        tiles = [trace_v[spot, piece(c), :].astype(jnp.bfloat16) for spot in (tile, tile + 1, last)]
        for h in range(2):
            pair = jnp.concatenate([tiles[h], tiles[h + 1]], axis=1)
            win[q, piece(c), pl.ds(h * LANES, LANES)] = jnp.dot(
                pair, moves[q], preferred_element_type=jnp.float32
            ).astype(jnp.bfloat16)

    def send(src, dst, send_sem, recv_sem, where):
        pltpu.make_async_remote_copy(
            src_ref=src, dst_ref=dst, send_sem=send_sem, recv_sem=recv_sem,
            device_id=where, device_id_type=MESH,
        ).start()

    def send_step(step, c):
        for cls in range(2):
            src = stack.at[gives[cls]] if step == 0 else sums.at[step - 1, cls]
            send(
                src.at[piece(c), :], land.at[step, cls, piece(c), :],
                z_send, z_recv.at[step, c],
                (slab, (second if step == 1 else first)[cls]),
            )

    def wait_step(step, c):
        wait_bytes(land.at[step, :, piece(c), :], z_recv.at[step, c])

    wait_bytes(trace_v, load_sem)
    tab_load.start()
    for c in range(CHUNKS):
        for q, o in enumerate([*OFFSETS, 0]):
            cut(q, o, c)
        if c == 0:
            pl.semaphore_wait(barrier, friends)

            @pl.when(jnp.logical_not(greets_side))
            def _():
                pl.semaphore_signal(
                    hello.at[0], inc=1, device_id=(slab, side), device_id_type=MESH
                )

            @pl.when(jnp.logical_not(greets_across))
            def _():
                pl.semaphore_signal(
                    hello.at[1], inc=1, device_id=(slab, across), device_id_type=MESH
                )

        for q, o in enumerate(OFFSETS):

            @pl.when(inside(slab + o))
            def _():
                if c == 0:
                    send(slots_out.at[q], slots_in.at[q], slot_send, slot_recv, (slab + o, det))
                send(
                    win.at[q, piece(c), :], got.at[q, piece(c), :],
                    win_send, win_recv.at[c], (slab + o, det),
                )

    wait_near(lambda n: slots_in.at[pl.ds(0, n)], slot_recv)
    for c in range(CHUNKS):
        wait_near(lambda n: got.at[pl.ds(0, n), piece(c), :], win_recv.at[c])

        rows = SIZES[c]
        for h in range(2):
            cols = pl.ds(h * LANES, LANES)
            bins = [jnp.zeros((rows, LANES), jnp.float32) for _ in range(NTAB)]
            for q, o in enumerate([*OFFSETS, 0]):
                source, slots = (win, slots_out) if o == 0 else (got, slots_in)
                window = source[q, piece(c), cols].astype(jnp.float32)
                block = jnp.broadcast_to(slots[q, 0:1, :], (rows, LANES))
                for t in range(NTAB):
                    bins[t] = bins[t] + jnp.where(block == t, window, 0.0)
            for t in range(NTAB):
                stack[t, piece(c), cols] = bins[t].astype(jnp.bfloat16)
        if c == 0:
            @pl.when(greets_side)
            def _():
                pl.semaphore_wait(hello.at[0], 1)

            @pl.when(greets_across)
            def _():
                pl.semaphore_wait(hello.at[1], 1)

        send_step(0, c)

    for step in range(2):
        for c in range(CHUNKS):
            wait_step(step, c)
            for cls in range(2):
                mine = stack[keeps[cls], piece(c), :] if step == 0 else sums[0, cls, piece(c), :]
                theirs = land[step, cls, piece(c), :]
                sums[step, cls, piece(c), :] = (
                    mine.astype(jnp.float32) + theirs.astype(jnp.float32)
                ).astype(jnp.bfloat16)
            send_step(step + 1, c)

    wait_bytes(tab, tab_sem)
    out_ref[...] = jnp.dot(
        sums[1, 0], tab[keeps[0]], preferred_element_type=jnp.float32
    ) + jnp.dot(sums[1, 1], tab[keeps[1]], preferred_element_type=jnp.float32)
    for c in range(CHUNKS):
        wait_step(2, c)
        total = out_ref[piece(c), :]
        for cls in range(2):
            total = total + jnp.dot(
                land[2, cls, piece(c), :], tab[gives[cls]], preferred_element_type=jnp.float32
            )
        out_ref[piece(c), :] = total

    wait_near(lambda n: slots_out.at[pl.ds(0, n)], slot_send)
    wait_near(lambda n: win.at[pl.ds(0, n)], win_send)
    wait_bytes(land, z_send)


def body(n_slab, traces, tables, slab_range, table_slot, sample_start):
    _, frames, samp = traces.shape
    vox = tables.shape[2]
    far = pl.BlockSpec(memory_space=pl.ANY)
    dma = pltpu.SemaphoreType.DMA
    return pl.pallas_call(
        functools.partial(kernel, n_slab),
        out_shape=pltpu.VMEM((frames, vox), jnp.float32),
        in_specs=[far] * 5,
        out_specs=pl.BlockSpec(memory_space=pltpu.VMEM),
        scratch_shapes=[
            pltpu.SMEM((1, 2), jnp.int32),
            pltpu.SMEM((1, REACH), jnp.int32),
            pltpu.SMEM((1, REACH), jnp.int32),
            pltpu.VMEM((samp // LANES, frames, LANES), jnp.float32),
            pltpu.VMEM((REACH, 2 * LANES, LANES), jnp.bfloat16),
            pltpu.VMEM((REACH, frames, KWIN), jnp.bfloat16),
            pltpu.VMEM((2 * RANGE, frames, KWIN), jnp.bfloat16),
            pltpu.VMEM((REACH, 8, LANES), jnp.int32),
            pltpu.VMEM((2 * RANGE, 8, LANES), jnp.int32),
            pltpu.VMEM((NTAB, frames, KWIN), jnp.bfloat16),
            pltpu.VMEM((2, 2, frames, KWIN), jnp.bfloat16),
            pltpu.VMEM((3, 2, frames, KWIN), jnp.bfloat16),
            pltpu.VMEM((NTAB, KWIN, vox), jnp.bfloat16),
            dma((3,)), dma, dma, dma, dma, dma, dma((CHUNKS,)), dma, dma((3, CHUNKS)),
            pltpu.SemaphoreType.REGULAR((2,)),
        ],
        compiler_params=pltpu.CompilerParams(collective_id=0, has_side_effects=True),
    )(traces, tables, slab_range, table_slot, sample_start)


def solution(mesh):
    placed = (
        P(("slab", "det"), None, None),
        P("slab", None, "det"),
        P(("slab", "det"), None),
        P(("slab", "det"), None),
        P(("slab", "det"), None),
    )
    return jax.shard_map(
        functools.partial(body, mesh.shape["slab"]),
        mesh=mesh, in_specs=placed, out_specs=P(None, ("slab", "det")), check_vma=False,
    )
```

```python
import functools

import jax
import jax.numpy as jnp
from jax import lax
from jax.experimental import pallas as pl
from jax.experimental.pallas import tpu as pltpu
from jax.sharding import PartitionSpec as P

KWIN = 256
NTAB = 4
RANGE = 3
REACH = 2 * RANGE + 1
SIZES = (16,) * 8
HEAD = 32
PLANE = 32
STEP = 24
DIRECT = 5
LAG = 1
CHUNKS = len(SIZES)
LANES = 128
MESH = pl.DeviceIdType.MESH
OFFSETS = [3, -3, 2, -2, 1, -1]


def kernel(
    n_slab, traces_ref, tables_ref, span_hbm, slot_hbm, start_hbm, out_ref,
    span_ref, slot_ref, start_ref, trace_a, trace_b, moves, win, got, slots_out, slots_in,
    stack, sums, land, tab, held,
    int_sem, load_sem, tab_sem, slot_send, slot_recv, win_send, win_recv, z_send, z_recv, hello,
    held_send, held_recv,
):
    slab = lax.axis_index("slab")
    det = lax.axis_index("det")
    side = det + 1 - 2 * lax.rem(det, 2)
    across = 3 - det
    keep_a = lax.rem((det + 1) // 2, 2)
    keep_b = 2 + det // 2
    first = (side, across)
    second = (across, side)
    keeps = (keep_a, keep_b)
    gives = (1 - keep_a, 5 - keep_b)
    n_tiles = trace_a.shape[0]
    near = jnp.minimum(slab, RANGE) + jnp.minimum(n_slab - 1 - slab, RANGE)

    def inside(s):
        return jnp.logical_and(s >= 0, s < n_slab)

    def piece(c):
        return pl.ds(sum(SIZES[:c]), SIZES[c])

    def leaves(s, o):
        return jnp.logical_and(inside(s + o), (s + o + PLANE) // PLANE != (s + PLANE) // PLANE)

    def aid(target, way):
        return target + way * STEP

    ways = (-1, 1)
    served = [slab - way * STEP for way in ways]
    passes = [
        [
            functools.reduce(
                jnp.logical_and,
                [
                    inside(served[w]),
                    (served[w] + PLANE) // PLANE == (slab + PLANE) // PLANE,
                    leaves(served[w], -way * a),
                ],
            )
            for a in range(1, RANGE + 1)
        ]
        for w, way in enumerate(ways)
    ]
    n_passes = [sum(p.astype(jnp.int32) for p in passes[w]) for w in range(2)]

    def wait_bytes(ref, sem):
        pltpu.make_async_copy(ref, ref, sem).wait()

    def wait_near(refs, sem):
        for n in range(RANGE, 2 * RANGE + 1):

            @pl.when(near == n)
            def _():
                wait_bytes(refs(n), sem)

    barrier = pltpu.get_barrier_semaphore()
    greets_side = jnp.logical_or(det == 0, det == 3)
    greets_across = det < 2
    friends = near + jnp.where(det == 2, 2, jnp.where(det == 0, 0, 1))
    for w in range(2):
        friends = friends + jnp.minimum(n_passes[w], 1)
    for o in OFFSETS:
        friends = friends + leaves(slab, o).astype(jnp.int32)

    @pl.when(greets_side)
    def _():
        pl.semaphore_signal(barrier, inc=1, device_id=(slab, side), device_id_type=MESH)

    @pl.when(greets_across)
    def _():
        pl.semaphore_signal(barrier, inc=1, device_id=(slab, across), device_id_type=MESH)

    for o in OFFSETS:

        @pl.when(inside(slab + o))
        def _():
            pl.semaphore_signal(barrier, inc=1, device_id=(slab + o, det), device_id_type=MESH)

    for w, way in enumerate(ways):

        @pl.when(leaves(slab, -way * RANGE))
        def _():
            pl.semaphore_signal(
                barrier, inc=1, device_id=(aid(slab, way), det), device_id_type=MESH
            )

        for a in range(1, RANGE + 1):

            @pl.when(passes[w][a - 1])
            def _():
                pl.semaphore_signal(
                    barrier, inc=1, device_id=(served[w] - way * a, det), device_id_type=MESH
                )

    ints = [
        pltpu.make_async_copy(src, dst, int_sem.at[n])
        for n, (src, dst) in enumerate(
            [(start_hbm, start_ref), (span_hbm, span_ref), (slot_hbm, slot_ref)]
        )
    ]
    for copy in ints:
        copy.start()

    for part, (buffer, top) in enumerate([(trace_a, 0), (trace_b, HEAD)]):

        @pl.loop(0, n_tiles)
        def _(tile):
            pltpu.make_async_copy(
                traces_ref.at[
                    0, pl.ds(top, buffer.shape[1]),
                    pl.ds(pl.multiple_of(tile * LANES, LANES), LANES),
                ],
                buffer.at[tile], load_sem.at[part],
            ).start()

    tab_load = pltpu.make_async_copy(tables_ref, tab, tab_sem)

    for copy in ints:
        copy.wait()

    flat = (8, LANES)
    low = jnp.full(flat, span_ref[0, 0], jnp.int32)
    high = jnp.full(flat, span_ref[0, 1], jnp.int32)
    for q, o in enumerate([*OFFSETS, 0]):
        target = slab + o
        active = jnp.logical_and(low <= target, target <= high)
        slots_out[q] = jnp.where(active, jnp.full(flat, slot_ref[0, o + RANGE], jnp.int32), -1)
    for q, o in enumerate(OFFSETS):

        @pl.when(jnp.logical_not(inside(slab - o)))
        def _():
            slots_in[q] = jnp.full(flat, -1, jnp.int32)
            got[q] = jnp.zeros(got.shape[1:], jnp.bfloat16)

    down = lax.broadcasted_iota(jnp.int32, (2 * LANES, LANES), 0)
    along = lax.broadcasted_iota(jnp.int32, (2 * LANES, LANES), 1)
    for q, o in enumerate([*OFFSETS, 0]):
        shift = lax.rem(start_ref[0, o + RANGE], LANES)
        moves[q] = jnp.where(down - along == shift, 1.0, 0.0).astype(jnp.bfloat16)

    def cut(q, o, c):
        tile = lax.div(start_ref[0, o + RANGE], LANES)
        last = lax.min(tile + 2, n_tiles - 1)
        top = sum(SIZES[:c])
        buffer, top = (trace_a, top) if top < HEAD else (trace_b, top - HEAD)
        tiles = [
            buffer[spot, pl.ds(top, SIZES[c]), :].astype(jnp.bfloat16)
            for spot in (tile, tile + 1, last)
        ]
        for h in range(2):
            pair = jnp.concatenate([tiles[h], tiles[h + 1]], axis=1)
            win[q, piece(c), pl.ds(h * LANES, LANES)] = jnp.dot(
                pair, moves[q], preferred_element_type=jnp.float32
            ).astype(jnp.bfloat16)

    def send(src, dst, send_sem, recv_sem, where):
        pltpu.make_async_remote_copy(
            src_ref=src, dst_ref=dst, send_sem=send_sem, recv_sem=recv_sem,
            device_id=where, device_id_type=MESH,
        ).start()

    def send_step(step, c):
        for cls in range(2):
            src = stack.at[gives[cls]] if step == 0 else sums.at[step - 1, cls]
            send(
                src.at[piece(c), :], land.at[step, cls, piece(c), :],
                z_send, z_recv.at[step, c],
                (slab, (second if step == 1 else first)[cls]),
            )

    def wait_step(step, c):
        wait_bytes(land.at[step, :, piece(c), :], z_recv.at[step, c])

    for c in range(CHUNKS):
        if c == 0:
            wait_bytes(trace_a, load_sem.at[0])
        if sum(SIZES[:c]) == HEAD:
            wait_bytes(trace_b, load_sem.at[1])
            tab_load.start()
        for q, o in enumerate([*OFFSETS, 0]):
            cut(q, o, c)
        if c == 0:
            pl.semaphore_wait(barrier, friends)

            @pl.when(jnp.logical_not(greets_side))
            def _():
                pl.semaphore_signal(
                    hello.at[0], inc=1, device_id=(slab, side), device_id_type=MESH
                )

            @pl.when(jnp.logical_not(greets_across))
            def _():
                pl.semaphore_signal(
                    hello.at[1], inc=1, device_id=(slab, across), device_id_type=MESH
                )

        for q, o in enumerate(OFFSETS):

            far = leaves(slab, o) if c >= DIRECT else False
            if c >= DIRECT:
                w, way = (0, -1) if o < 0 else (1, 1)

                @pl.when(far)
                def _():
                    send(
                        win.at[q, piece(c), :], held.at[w, abs(o) - 1, piece(c), :],
                        win_send, held_recv.at[w, c - DIRECT], (aid(slab + o, way), det),
                    )

            @pl.when(jnp.logical_and(inside(slab + o), jnp.logical_not(far)))
            def _():
                if c == 0:
                    send(slots_out.at[q], slots_in.at[q], slot_send, slot_recv, (slab + o, det))
                send(
                    win.at[q, piece(c), :], got.at[q, piece(c), :],
                    win_send, win_recv.at[c], (slab + o, det),
                )

    def pass_on(c):
        for w, way in enumerate(ways):
            for n in range(1, RANGE + 1):

                @pl.when(n_passes[w] == n)
                def _():
                    wait_bytes(held.at[w, pl.ds(0, n), piece(c), :], held_recv.at[w, c - DIRECT])

            for a in range(1, RANGE + 1):

                @pl.when(passes[w][a - 1])
                def _():
                    send(
                        held.at[w, a - 1, piece(c), :],
                        got.at[OFFSETS.index(way * a), piece(c), :],
                        held_send, win_recv.at[c], (served[w], det),
                    )

    wait_near(lambda n: slots_in.at[pl.ds(0, n)], slot_recv)
    for c in range(CHUNKS):
        wait_near(lambda n: got.at[pl.ds(0, n), piece(c), :], win_recv.at[c])

        rows = SIZES[c]
        for h in range(2):
            cols = pl.ds(h * LANES, LANES)
            bins = [jnp.zeros((rows, LANES), jnp.float32) for _ in range(NTAB)]
            for q, o in enumerate([*OFFSETS, 0]):
                source, slots = (win, slots_out) if o == 0 else (got, slots_in)
                window = source[q, piece(c), cols].astype(jnp.float32)
                block = jnp.broadcast_to(slots[q, 0:1, :], (rows, LANES))
                for t in range(NTAB):
                    bins[t] = bins[t] + jnp.where(block == t, window, 0.0)
            for t in range(NTAB):
                stack[t, piece(c), cols] = bins[t].astype(jnp.bfloat16)
        if c == 0:
            @pl.when(greets_side)
            def _():
                pl.semaphore_wait(hello.at[0], 1)

            @pl.when(greets_across)
            def _():
                pl.semaphore_wait(hello.at[1], 1)

        send_step(0, c)
        for late in range(DIRECT, CHUNKS):
            if c == min(late + LAG, CHUNKS - 1):
                pass_on(late)

    for step in range(2):
        for c in range(CHUNKS):
            wait_step(step, c)
            for cls in range(2):
                mine = stack[keeps[cls], piece(c), :] if step == 0 else sums[0, cls, piece(c), :]
                theirs = land[step, cls, piece(c), :]
                sums[step, cls, piece(c), :] = (
                    mine.astype(jnp.float32) + theirs.astype(jnp.float32)
                ).astype(jnp.bfloat16)
            send_step(step + 1, c)

    wait_bytes(tab, tab_sem)
    out_ref[...] = jnp.dot(
        sums[1, 0], tab[keeps[0]], preferred_element_type=jnp.float32
    ) + jnp.dot(sums[1, 1], tab[keeps[1]], preferred_element_type=jnp.float32)
    for c in range(CHUNKS):
        wait_step(2, c)
        total = out_ref[piece(c), :]
        for cls in range(2):
            total = total + jnp.dot(
                land[2, cls, piece(c), :], tab[gives[cls]], preferred_element_type=jnp.float32
            )
        out_ref[piece(c), :] = total

    wait_near(lambda n: slots_out.at[pl.ds(0, n)], slot_send)
    wait_near(lambda n: win.at[pl.ds(0, n)], win_send)
    wait_bytes(land, z_send)
    for w in range(2):
        for n in range(1, RANGE + 1):

            @pl.when(n_passes[w] == n)
            def _():
                passed = pl.ds(sum(SIZES[:DIRECT]), sum(SIZES[DIRECT:]))
                wait_bytes(held.at[w, pl.ds(0, n), passed, :], held_send)


def body(n_slab, traces, tables, slab_range, table_slot, sample_start):
    _, frames, samp = traces.shape
    vox = tables.shape[2]
    far = pl.BlockSpec(memory_space=pl.ANY)
    dma = pltpu.SemaphoreType.DMA
    return pl.pallas_call(
        functools.partial(kernel, n_slab),
        out_shape=pltpu.VMEM((frames, vox), jnp.float32),
        in_specs=[far] * 5,
        out_specs=pl.BlockSpec(memory_space=pltpu.VMEM),
        scratch_shapes=[
            pltpu.SMEM((1, 2), jnp.int32),
            pltpu.SMEM((1, REACH), jnp.int32),
            pltpu.SMEM((1, REACH), jnp.int32),
            pltpu.VMEM((samp // LANES, HEAD, LANES), jnp.float32),
            pltpu.VMEM((samp // LANES, frames - HEAD, LANES), jnp.float32),
            pltpu.VMEM((REACH, 2 * LANES, LANES), jnp.bfloat16),
            pltpu.VMEM((REACH, frames, KWIN), jnp.bfloat16),
            pltpu.VMEM((2 * RANGE, frames, KWIN), jnp.bfloat16),
            pltpu.VMEM((REACH, 8, LANES), jnp.int32),
            pltpu.VMEM((2 * RANGE, 8, LANES), jnp.int32),
            pltpu.VMEM((NTAB, frames, KWIN), jnp.bfloat16),
            pltpu.VMEM((2, 2, frames, KWIN), jnp.bfloat16),
            pltpu.VMEM((3, 2, frames, KWIN), jnp.bfloat16),
            pltpu.VMEM((NTAB, KWIN, vox), jnp.bfloat16),
            pltpu.VMEM((2, RANGE, frames, KWIN), jnp.bfloat16),
            dma((3,)), dma((2,)), dma, dma, dma, dma, dma((CHUNKS,)), dma, dma((3, CHUNKS)),
            pltpu.SemaphoreType.REGULAR((2,)),
            dma, dma((2, CHUNKS - DIRECT)),
        ],
        compiler_params=pltpu.CompilerParams(collective_id=0, has_side_effects=True),
    )(traces, tables, slab_range, table_slot, sample_start)


def solution(mesh):
    placed = (
        P(("slab", "det"), None, None),
        P("slab", None, "det"),
        P(("slab", "det"), None),
        P(("slab", "det"), None),
        P(("slab", "det"), None),
    )
    return jax.shard_map(
        functools.partial(body, mesh.shape["slab"]),
        mesh=mesh, in_specs=placed, out_specs=P(None, ("slab", "det")), check_vma=False,
    )
```

```python
import functools

import jax
import jax.numpy as jnp
from jax import lax
from jax.experimental import pallas as pl
from jax.experimental.pallas import tpu as pltpu
from jax.sharding import PartitionSpec as P

KWIN = 256
NTAB = 4
RANGE = 3
REACH = 2 * RANGE + 1
SIZES = (16,) * 8
HEAD = 32
PLANE = 32
STEP = 24
DIRECT = 5
LAG = 0
CHUNKS = len(SIZES)
LANES = 128
SUB = 8
MESH = pl.DeviceIdType.MESH
OFFSETS = [3, -3, 2, -2, 1, -1]


def kernel(
    n_slab, traces_ref, tables_ref, span_hbm, slot_hbm, start_hbm, out_ref,
    span_ref, slot_ref, start_ref, trace_a, trace_b, moves, win, got, slots_out, slots_in,
    stack, sums, land, tab, held,
    int_sem, load_sem, tab_sem, slot_send, slot_recv, win_send, win_recv, z_send, z_recv, hello,
    held_send, held_recv,
):
    slab = lax.axis_index("slab")
    det = lax.axis_index("det")
    side = det + 1 - 2 * lax.rem(det, 2)
    across = 3 - det
    keep_a = lax.rem((det + 1) // 2, 2)
    keep_b = 2 + det // 2
    first = (side, across)
    second = (across, side)
    keeps = (keep_a, keep_b)
    gives = (1 - keep_a, 5 - keep_b)
    n_tiles = trace_a.shape[1]
    near = jnp.minimum(slab, RANGE) + jnp.minimum(n_slab - 1 - slab, RANGE)

    def inside(s):
        return jnp.logical_and(s >= 0, s < n_slab)

    def piece(c):
        return pl.ds(sum(SIZES[:c]), SIZES[c])

    def leaves(s, o):
        return jnp.logical_and(inside(s + o), (s + o + PLANE) // PLANE != (s + PLANE) // PLANE)

    def aid(target, way):
        return target + way * STEP

    ways = (-1, 1)
    served = [slab - way * STEP for way in ways]
    passes = [
        [
            functools.reduce(
                jnp.logical_and,
                [
                    inside(served[w]),
                    (served[w] + PLANE) // PLANE == (slab + PLANE) // PLANE,
                    leaves(served[w], -way * a),
                ],
            )
            for a in range(1, RANGE + 1)
        ]
        for w, way in enumerate(ways)
    ]
    n_passes = [sum(p.astype(jnp.int32) for p in passes[w]) for w in range(2)]

    def wait_bytes(ref, sem):
        pltpu.make_async_copy(ref, ref, sem).wait()

    def wait_near(refs, sem):
        for n in range(RANGE, 2 * RANGE + 1):

            @pl.when(near == n)
            def _():
                wait_bytes(refs(n), sem)

    barrier = pltpu.get_barrier_semaphore()
    greets_side = jnp.logical_or(det == 0, det == 3)
    greets_across = det < 2
    friends = near + jnp.where(det == 2, 2, jnp.where(det == 0, 0, 1))
    for w in range(2):
        friends = friends + jnp.minimum(n_passes[w], 1)
    for o in OFFSETS:
        friends = friends + leaves(slab, o).astype(jnp.int32)

    @pl.when(greets_side)
    def _():
        pl.semaphore_signal(barrier, inc=1, device_id=(slab, side), device_id_type=MESH)

    @pl.when(greets_across)
    def _():
        pl.semaphore_signal(barrier, inc=1, device_id=(slab, across), device_id_type=MESH)

    for o in OFFSETS:

        @pl.when(inside(slab + o))
        def _():
            pl.semaphore_signal(barrier, inc=1, device_id=(slab + o, det), device_id_type=MESH)

    for w, way in enumerate(ways):

        @pl.when(leaves(slab, -way * RANGE))
        def _():
            pl.semaphore_signal(
                barrier, inc=1, device_id=(aid(slab, way), det), device_id_type=MESH
            )

        for a in range(1, RANGE + 1):

            @pl.when(passes[w][a - 1])
            def _():
                pl.semaphore_signal(
                    barrier, inc=1, device_id=(served[w] - way * a, det), device_id_type=MESH
                )

    ints = [
        pltpu.make_async_copy(src, dst, int_sem.at[n])
        for n, (src, dst) in enumerate(
            [(start_hbm, start_ref), (span_hbm, span_ref), (slot_hbm, slot_ref)]
        )
    ]
    for copy in ints:
        copy.start()

    loads = [
        pltpu.make_async_copy(
            traces_ref.at[pl.ds(top // SUB, buffer.shape[0])], buffer, load_sem.at[part]
        )
        for part, (buffer, top) in enumerate([(trace_a, 0), (trace_b, HEAD)])
    ]
    for load in loads:
        load.start()
    tab_load = pltpu.make_async_copy(tables_ref, tab, tab_sem)

    for copy in ints:
        copy.wait()

    flat = (8, LANES)
    low = jnp.full(flat, span_ref[0, 0], jnp.int32)
    high = jnp.full(flat, span_ref[0, 1], jnp.int32)
    for q, o in enumerate([*OFFSETS, 0]):
        target = slab + o
        active = jnp.logical_and(low <= target, target <= high)
        slots_out[q] = jnp.where(active, jnp.full(flat, slot_ref[0, o + RANGE], jnp.int32), -1)
    for q, o in enumerate(OFFSETS):

        @pl.when(jnp.logical_not(inside(slab - o)))
        def _():
            slots_in[q] = jnp.full(flat, -1, jnp.int32)
            got[q] = jnp.zeros(got.shape[1:], jnp.bfloat16)

    down = lax.broadcasted_iota(jnp.int32, (2 * LANES, LANES), 0)
    along = lax.broadcasted_iota(jnp.int32, (2 * LANES, LANES), 1)
    for q, o in enumerate([*OFFSETS, 0]):
        shift = lax.rem(start_ref[0, o + RANGE], LANES)
        moves[q] = jnp.where(down - along == shift, 1.0, 0.0).astype(jnp.bfloat16)

    def cut(q, o, c):
        tile = lax.div(start_ref[0, o + RANGE], LANES)
        last = lax.min(tile + 2, n_tiles - 1)
        top = sum(SIZES[:c])
        buffer, top = (trace_a, top) if top < HEAD else (trace_b, top - HEAD)
        tiles = [
            buffer[pl.ds(top // SUB, SIZES[c] // SUB), spot]
            .reshape(SIZES[c], LANES)
            .astype(jnp.bfloat16)
            for spot in (tile, tile + 1, last)
        ]
        for h in range(2):
            pair = jnp.concatenate([tiles[h], tiles[h + 1]], axis=1)
            win[q, piece(c), pl.ds(h * LANES, LANES)] = jnp.dot(
                pair, moves[q], preferred_element_type=jnp.float32
            ).astype(jnp.bfloat16)

    def send(src, dst, send_sem, recv_sem, where):
        pltpu.make_async_remote_copy(
            src_ref=src, dst_ref=dst, send_sem=send_sem, recv_sem=recv_sem,
            device_id=where, device_id_type=MESH,
        ).start()

    def send_step(step, c):
        for cls in range(2):
            src = stack.at[gives[cls]] if step == 0 else sums.at[step - 1, cls]
            send(
                src.at[piece(c), :], land.at[step, cls, piece(c), :],
                z_send, z_recv.at[step, c],
                (slab, (second if step == 1 else first)[cls]),
            )

    def wait_step(step, c):
        wait_bytes(land.at[step, :, piece(c), :], z_recv.at[step, c])

    for c in range(CHUNKS):
        if c == 0:
            loads[0].wait()
        if sum(SIZES[:c]) == HEAD:
            loads[1].wait()
            tab_load.start()
        for q, o in enumerate([*OFFSETS, 0]):
            cut(q, o, c)
        if c == 0:
            pl.semaphore_wait(barrier, friends)

            @pl.when(jnp.logical_not(greets_side))
            def _():
                pl.semaphore_signal(
                    hello.at[0], inc=1, device_id=(slab, side), device_id_type=MESH
                )

            @pl.when(jnp.logical_not(greets_across))
            def _():
                pl.semaphore_signal(
                    hello.at[1], inc=1, device_id=(slab, across), device_id_type=MESH
                )

        for q, o in enumerate(OFFSETS):

            far = leaves(slab, o) if c >= DIRECT else False
            if c >= DIRECT:
                w, way = (0, -1) if o < 0 else (1, 1)

                @pl.when(far)
                def _():
                    send(
                        win.at[q, piece(c), :], held.at[w, abs(o) - 1, piece(c), :],
                        win_send, held_recv.at[w, c - DIRECT], (aid(slab + o, way), det),
                    )

            @pl.when(jnp.logical_and(inside(slab + o), jnp.logical_not(far)))
            def _():
                if c == 0:
                    send(slots_out.at[q], slots_in.at[q], slot_send, slot_recv, (slab + o, det))
                send(
                    win.at[q, piece(c), :], got.at[q, piece(c), :],
                    win_send, win_recv.at[c], (slab + o, det),
                )

    def pass_on(c):
        for w, way in enumerate(ways):
            for n in range(1, RANGE + 1):

                @pl.when(n_passes[w] == n)
                def _():
                    wait_bytes(held.at[w, pl.ds(0, n), piece(c), :], held_recv.at[w, c - DIRECT])

            for a in range(1, RANGE + 1):

                @pl.when(passes[w][a - 1])
                def _():
                    send(
                        held.at[w, a - 1, piece(c), :],
                        got.at[OFFSETS.index(way * a), piece(c), :],
                        held_send, win_recv.at[c], (served[w], det),
                    )

    wait_near(lambda n: slots_in.at[pl.ds(0, n)], slot_recv)
    for c in range(CHUNKS):
        wait_near(lambda n: got.at[pl.ds(0, n), piece(c), :], win_recv.at[c])

        rows = SIZES[c]
        for h in range(2):
            cols = pl.ds(h * LANES, LANES)
            bins = [jnp.zeros((rows, LANES), jnp.float32) for _ in range(NTAB)]
            for q, o in enumerate([*OFFSETS, 0]):
                source, slots = (win, slots_out) if o == 0 else (got, slots_in)
                window = source[q, piece(c), cols].astype(jnp.float32)
                block = jnp.broadcast_to(slots[q, 0:1, :], (rows, LANES))
                for t in range(NTAB):
                    bins[t] = bins[t] + jnp.where(block == t, window, 0.0)
            for t in range(NTAB):
                stack[t, piece(c), cols] = bins[t].astype(jnp.bfloat16)
        if c == 0:
            @pl.when(greets_side)
            def _():
                pl.semaphore_wait(hello.at[0], 1)

            @pl.when(greets_across)
            def _():
                pl.semaphore_wait(hello.at[1], 1)

        send_step(0, c)
        for late in range(DIRECT, CHUNKS):
            if c == min(late + LAG, CHUNKS - 1):
                pass_on(late)

    for step in range(2):
        for c in range(CHUNKS):
            wait_step(step, c)
            for cls in range(2):
                mine = stack[keeps[cls], piece(c), :] if step == 0 else sums[0, cls, piece(c), :]
                theirs = land[step, cls, piece(c), :]
                sums[step, cls, piece(c), :] = (
                    mine.astype(jnp.float32) + theirs.astype(jnp.float32)
                ).astype(jnp.bfloat16)
            send_step(step + 1, c)

    wait_bytes(tab, tab_sem)
    out_ref[...] = jnp.dot(
        sums[1, 0], tab[keeps[0]], preferred_element_type=jnp.float32
    ) + jnp.dot(sums[1, 1], tab[keeps[1]], preferred_element_type=jnp.float32)
    for c in range(CHUNKS):
        wait_step(2, c)
        total = out_ref[piece(c), :]
        for cls in range(2):
            total = total + jnp.dot(
                land[2, cls, piece(c), :], tab[gives[cls]], preferred_element_type=jnp.float32
            )
        out_ref[piece(c), :] = total

    wait_near(lambda n: slots_out.at[pl.ds(0, n)], slot_send)
    wait_near(lambda n: win.at[pl.ds(0, n)], win_send)
    wait_bytes(land, z_send)
    for w in range(2):
        for n in range(1, RANGE + 1):

            @pl.when(n_passes[w] == n)
            def _():
                passed = pl.ds(sum(SIZES[:DIRECT]), sum(SIZES[DIRECT:]))
                wait_bytes(held.at[w, pl.ds(0, n), passed, :], held_send)


def body(n_slab, traces, tables, slab_range, table_slot, sample_start):
    _, frames, samp = traces.shape
    vox = tables.shape[2]
    traces = traces.reshape(frames // SUB, SUB, samp // LANES, LANES).transpose(0, 2, 1, 3)
    far = pl.BlockSpec(memory_space=pl.ANY)
    dma = pltpu.SemaphoreType.DMA
    return pl.pallas_call(
        functools.partial(kernel, n_slab),
        out_shape=pltpu.VMEM((frames, vox), jnp.float32),
        in_specs=[far] * 5,
        out_specs=pl.BlockSpec(memory_space=pltpu.VMEM),
        scratch_shapes=[
            pltpu.SMEM((1, 2), jnp.int32),
            pltpu.SMEM((1, REACH), jnp.int32),
            pltpu.SMEM((1, REACH), jnp.int32),
            pltpu.VMEM((HEAD // SUB, samp // LANES, SUB, LANES), jnp.float32),
            pltpu.VMEM(((frames - HEAD) // SUB, samp // LANES, SUB, LANES), jnp.float32),
            pltpu.VMEM((REACH, 2 * LANES, LANES), jnp.bfloat16),
            pltpu.VMEM((REACH, frames, KWIN), jnp.bfloat16),
            pltpu.VMEM((2 * RANGE, frames, KWIN), jnp.bfloat16),
            pltpu.VMEM((REACH, 8, LANES), jnp.int32),
            pltpu.VMEM((2 * RANGE, 8, LANES), jnp.int32),
            pltpu.VMEM((NTAB, frames, KWIN), jnp.bfloat16),
            pltpu.VMEM((2, 2, frames, KWIN), jnp.bfloat16),
            pltpu.VMEM((3, 2, frames, KWIN), jnp.bfloat16),
            pltpu.VMEM((NTAB, KWIN, vox), jnp.bfloat16),
            pltpu.VMEM((2, RANGE, frames, KWIN), jnp.bfloat16),
            dma((3,)), dma((2,)), dma, dma, dma, dma, dma((CHUNKS,)), dma, dma((3, CHUNKS)),
            pltpu.SemaphoreType.REGULAR((2,)),
            dma, dma((2, CHUNKS - DIRECT)),
        ],
        compiler_params=pltpu.CompilerParams(collective_id=0, has_side_effects=True),
    )(traces, tables, slab_range, table_slot, sample_start)


def solution(mesh):
    placed = (
        P(("slab", "det"), None, None),
        P("slab", None, "det"),
        P(("slab", "det"), None),
        P(("slab", "det"), None),
        P(("slab", "det"), None),
    )
    return jax.shard_map(
        functools.partial(body, mesh.shape["slab"]),
        mesh=mesh, in_specs=placed, out_specs=P(None, ("slab", "det")), check_vma=False,
    )
```

```python
import functools

import jax
import jax.numpy as jnp
from jax import lax
from jax.experimental import pallas as pl
from jax.experimental.pallas import tpu as pltpu
from jax.sharding import PartitionSpec as P

KWIN = 256
NTAB = 4
RANGE = 3
REACH = 2 * RANGE + 1
SIZES = (16,) * 8
HEAD = 32
PLANE = 32
STEP = 24
DIRECT = 5
LAG = 0
CHUNKS = len(SIZES)
LANES = 128
SUB = 8
MESH = pl.DeviceIdType.MESH
OFFSETS = [3, -3, 2, -2, 1, -1]


def kernel(
    n_slab, traces_ref, tables_ref, span_hbm, slot_hbm, start_hbm, out_ref,
    span_ref, slot_ref, start_ref, trace_a, trace_b, moves, win, got, slots_out, slots_in,
    stack, sums, land, tab, held,
    int_sem, load_sem, tab_sem, slot_send, slot_recv, win_send, win_recv, z_send, z_recv, z_last, hello,
    held_send, held_recv,
):
    slab = lax.axis_index("slab")
    det = lax.axis_index("det")
    side = det + 1 - 2 * lax.rem(det, 2)
    across = 3 - det
    keep_a = lax.rem((det + 1) // 2, 2)
    keep_b = 2 + det // 2
    first = (side, across)
    second = (across, side)
    keeps = (keep_a, keep_b)
    gives = (1 - keep_a, 5 - keep_b)
    n_tiles = trace_a.shape[1]
    near = jnp.minimum(slab, RANGE) + jnp.minimum(n_slab - 1 - slab, RANGE)

    def inside(s):
        return jnp.logical_and(s >= 0, s < n_slab)

    def piece(c):
        return pl.ds(sum(SIZES[:c]), SIZES[c])

    def leaves(s, o):
        return jnp.logical_and(inside(s + o), (s + o + PLANE) // PLANE != (s + PLANE) // PLANE)

    def aid(target, way):
        return target + way * STEP

    ways = (-1, 1)
    served = [slab - way * STEP for way in ways]
    passes = [
        [
            functools.reduce(
                jnp.logical_and,
                [
                    inside(served[w]),
                    (served[w] + PLANE) // PLANE == (slab + PLANE) // PLANE,
                    leaves(served[w], -way * a),
                ],
            )
            for a in range(1, RANGE + 1)
        ]
        for w, way in enumerate(ways)
    ]
    n_passes = [sum(p.astype(jnp.int32) for p in passes[w]) for w in range(2)]

    def wait_bytes(ref, sem):
        pltpu.make_async_copy(ref, ref, sem).wait()

    def wait_near(refs, sem):
        for n in range(RANGE, 2 * RANGE + 1):

            @pl.when(near == n)
            def _():
                wait_bytes(refs(n), sem)

    barrier = pltpu.get_barrier_semaphore()
    greets_side = jnp.logical_or(det == 0, det == 3)
    greets_across = det < 2
    friends = near + jnp.where(det == 2, 2, jnp.where(det == 0, 0, 1))
    for w in range(2):
        friends = friends + jnp.minimum(n_passes[w], 1)
    for o in OFFSETS:
        friends = friends + leaves(slab, o).astype(jnp.int32)

    @pl.when(greets_side)
    def _():
        pl.semaphore_signal(barrier, inc=1, device_id=(slab, side), device_id_type=MESH)

    @pl.when(greets_across)
    def _():
        pl.semaphore_signal(barrier, inc=1, device_id=(slab, across), device_id_type=MESH)

    for o in OFFSETS:

        @pl.when(inside(slab + o))
        def _():
            pl.semaphore_signal(barrier, inc=1, device_id=(slab + o, det), device_id_type=MESH)

    for w, way in enumerate(ways):

        @pl.when(leaves(slab, -way * RANGE))
        def _():
            pl.semaphore_signal(
                barrier, inc=1, device_id=(aid(slab, way), det), device_id_type=MESH
            )

        for a in range(1, RANGE + 1):

            @pl.when(passes[w][a - 1])
            def _():
                pl.semaphore_signal(
                    barrier, inc=1, device_id=(served[w] - way * a, det), device_id_type=MESH
                )

    ints = [
        pltpu.make_async_copy(src, dst, int_sem.at[n])
        for n, (src, dst) in enumerate(
            [(start_hbm, start_ref), (span_hbm, span_ref), (slot_hbm, slot_ref)]
        )
    ]
    for copy in ints:
        copy.start()

    loads = [
        pltpu.make_async_copy(
            traces_ref.at[pl.ds(top // SUB, buffer.shape[0])], buffer, load_sem.at[part]
        )
        for part, (buffer, top) in enumerate([(trace_a, 0), (trace_b, HEAD)])
    ]
    for load in loads:
        load.start()
    tab_load = pltpu.make_async_copy(tables_ref, tab, tab_sem)

    for copy in ints:
        copy.wait()

    flat = (8, LANES)
    low = jnp.full(flat, span_ref[0, 0], jnp.int32)
    high = jnp.full(flat, span_ref[0, 1], jnp.int32)
    for q, o in enumerate([*OFFSETS, 0]):
        target = slab + o
        active = jnp.logical_and(low <= target, target <= high)
        slots_out[q] = jnp.where(active, jnp.full(flat, slot_ref[0, o + RANGE], jnp.int32), -1)
    for q, o in enumerate(OFFSETS):

        @pl.when(jnp.logical_not(inside(slab - o)))
        def _():
            slots_in[q] = jnp.full(flat, -1, jnp.int32)
            got[q] = jnp.zeros(got.shape[1:], jnp.bfloat16)

    down = lax.broadcasted_iota(jnp.int32, (2 * LANES, LANES), 0)
    along = lax.broadcasted_iota(jnp.int32, (2 * LANES, LANES), 1)
    for q, o in enumerate([*OFFSETS, 0]):
        shift = lax.rem(start_ref[0, o + RANGE], LANES)
        moves[q] = jnp.where(down - along == shift, 1.0, 0.0).astype(jnp.bfloat16)

    def cut(q, o, c):
        tile = lax.div(start_ref[0, o + RANGE], LANES)
        last = lax.min(tile + 2, n_tiles - 1)
        top = sum(SIZES[:c])
        buffer, top = (trace_a, top) if top < HEAD else (trace_b, top - HEAD)
        tiles = [
            buffer[pl.ds(top // SUB, SIZES[c] // SUB), spot]
            .reshape(SIZES[c], LANES)
            .astype(jnp.bfloat16)
            for spot in (tile, tile + 1, last)
        ]
        for h in range(2):
            pair = jnp.concatenate([tiles[h], tiles[h + 1]], axis=1)
            win[q, piece(c), pl.ds(h * LANES, LANES)] = jnp.dot(
                pair, moves[q], preferred_element_type=jnp.float32
            ).astype(jnp.bfloat16)

    def send(src, dst, send_sem, recv_sem, where):
        pltpu.make_async_remote_copy(
            src_ref=src, dst_ref=dst, send_sem=send_sem, recv_sem=recv_sem,
            device_id=where, device_id_type=MESH,
        ).start()

    def send_step(step, c):
        for cls in range(2):
            src = stack.at[gives[cls]] if step == 0 else sums.at[step - 1, cls]
            send(
                src.at[piece(c), :], land.at[step, cls, piece(c), :],
                z_send, z_last.at[c // 2] if step == 2 else z_recv.at[step, c],
                (slab, (second if step == 1 else first)[cls]),
            )

    def wait_step(step, c):
        wait_bytes(land.at[step, :, piece(c), :], z_recv.at[step, c])

    for c in range(CHUNKS):
        if c == 0:
            loads[0].wait()
        if sum(SIZES[:c]) == HEAD:
            loads[1].wait()
            tab_load.start()
        for q, o in enumerate([*OFFSETS, 0]):
            cut(q, o, c)
        if c == 0:
            pl.semaphore_wait(barrier, friends)

            @pl.when(jnp.logical_not(greets_side))
            def _():
                pl.semaphore_signal(
                    hello.at[0], inc=1, device_id=(slab, side), device_id_type=MESH
                )

            @pl.when(jnp.logical_not(greets_across))
            def _():
                pl.semaphore_signal(
                    hello.at[1], inc=1, device_id=(slab, across), device_id_type=MESH
                )

        for q, o in enumerate(OFFSETS):

            far = leaves(slab, o) if c >= DIRECT else False
            if c >= DIRECT:
                w, way = (0, -1) if o < 0 else (1, 1)

                @pl.when(far)
                def _():
                    send(
                        win.at[q, piece(c), :], held.at[w, abs(o) - 1, piece(c), :],
                        win_send, held_recv.at[w, c - DIRECT], (aid(slab + o, way), det),
                    )

            @pl.when(jnp.logical_and(inside(slab + o), jnp.logical_not(far)))
            def _():
                if c == 0:
                    send(slots_out.at[q], slots_in.at[q], slot_send, slot_recv, (slab + o, det))
                send(
                    win.at[q, piece(c), :], got.at[q, piece(c), :],
                    win_send, win_recv.at[c], (slab + o, det),
                )

    def pass_on(c):
        for w, way in enumerate(ways):
            for n in range(1, RANGE + 1):

                @pl.when(n_passes[w] == n)
                def _():
                    wait_bytes(held.at[w, pl.ds(0, n), piece(c), :], held_recv.at[w, c - DIRECT])

            for a in range(1, RANGE + 1):

                @pl.when(passes[w][a - 1])
                def _():
                    send(
                        held.at[w, a - 1, piece(c), :],
                        got.at[OFFSETS.index(way * a), piece(c), :],
                        held_send, win_recv.at[c], (served[w], det),
                    )

    wait_near(lambda n: slots_in.at[pl.ds(0, n)], slot_recv)
    for c in range(CHUNKS):
        wait_near(lambda n: got.at[pl.ds(0, n), piece(c), :], win_recv.at[c])

        rows = SIZES[c]
        for h in range(2):
            cols = pl.ds(h * LANES, LANES)
            bins = [jnp.zeros((rows, LANES), jnp.float32) for _ in range(NTAB)]
            for q, o in enumerate([*OFFSETS, 0]):
                source, slots = (win, slots_out) if o == 0 else (got, slots_in)
                window = source[q, piece(c), cols].astype(jnp.float32)
                block = jnp.broadcast_to(slots[q, 0:1, :], (rows, LANES))
                for t in range(NTAB):
                    bins[t] = bins[t] + jnp.where(block == t, window, 0.0)
            for t in range(NTAB):
                stack[t, piece(c), cols] = bins[t].astype(jnp.bfloat16)
        if c == 0:
            @pl.when(greets_side)
            def _():
                pl.semaphore_wait(hello.at[0], 1)

            @pl.when(greets_across)
            def _():
                pl.semaphore_wait(hello.at[1], 1)

        send_step(0, c)
        for late in range(DIRECT, CHUNKS):
            if c == min(late + LAG, CHUNKS - 1):
                pass_on(late)

    for step in range(2):
        for c in range(CHUNKS):
            wait_step(step, c)
            for cls in range(2):
                mine = stack[keeps[cls], piece(c), :] if step == 0 else sums[0, cls, piece(c), :]
                theirs = land[step, cls, piece(c), :]
                sums[step, cls, piece(c), :] = (
                    mine.astype(jnp.float32) + theirs.astype(jnp.float32)
                ).astype(jnp.bfloat16)
            send_step(step + 1, c)

    wait_bytes(tab, tab_sem)
    out_ref[...] = jnp.dot(
        sums[1, 0], tab[keeps[0]], preferred_element_type=jnp.float32
    ) + jnp.dot(sums[1, 1], tab[keeps[1]], preferred_element_type=jnp.float32)
    for pair in range(CHUNKS // 2):
        both = pl.ds(sum(SIZES[: 2 * pair]), SIZES[2 * pair] + SIZES[2 * pair + 1])
        wait_bytes(land.at[2, :, both, :], z_last.at[pair])
        total = out_ref[both, :]
        for cls in range(2):
            total = total + jnp.dot(
                land[2, cls, both, :], tab[gives[cls]], preferred_element_type=jnp.float32
            )
        out_ref[both, :] = total

    wait_near(lambda n: slots_out.at[pl.ds(0, n)], slot_send)
    wait_near(lambda n: win.at[pl.ds(0, n)], win_send)
    wait_bytes(land, z_send)
    for w in range(2):
        for n in range(1, RANGE + 1):

            @pl.when(n_passes[w] == n)
            def _():
                passed = pl.ds(sum(SIZES[:DIRECT]), sum(SIZES[DIRECT:]))
                wait_bytes(held.at[w, pl.ds(0, n), passed, :], held_send)


def body(n_slab, traces, tables, slab_range, table_slot, sample_start):
    _, frames, samp = traces.shape
    vox = tables.shape[2]
    traces = traces.reshape(frames // SUB, SUB, samp // LANES, LANES).transpose(0, 2, 1, 3)
    far = pl.BlockSpec(memory_space=pl.ANY)
    dma = pltpu.SemaphoreType.DMA
    return pl.pallas_call(
        functools.partial(kernel, n_slab),
        out_shape=pltpu.VMEM((frames, vox), jnp.float32),
        in_specs=[far] * 5,
        out_specs=pl.BlockSpec(memory_space=pltpu.VMEM),
        scratch_shapes=[
            pltpu.SMEM((1, 2), jnp.int32),
            pltpu.SMEM((1, REACH), jnp.int32),
            pltpu.SMEM((1, REACH), jnp.int32),
            pltpu.VMEM((HEAD // SUB, samp // LANES, SUB, LANES), jnp.float32),
            pltpu.VMEM(((frames - HEAD) // SUB, samp // LANES, SUB, LANES), jnp.float32),
            pltpu.VMEM((REACH, 2 * LANES, LANES), jnp.bfloat16),
            pltpu.VMEM((REACH, frames, KWIN), jnp.bfloat16),
            pltpu.VMEM((2 * RANGE, frames, KWIN), jnp.bfloat16),
            pltpu.VMEM((REACH, 8, LANES), jnp.int32),
            pltpu.VMEM((2 * RANGE, 8, LANES), jnp.int32),
            pltpu.VMEM((NTAB, frames, KWIN), jnp.bfloat16),
            pltpu.VMEM((2, 2, frames, KWIN), jnp.bfloat16),
            pltpu.VMEM((3, 2, frames, KWIN), jnp.bfloat16),
            pltpu.VMEM((NTAB, KWIN, vox), jnp.bfloat16),
            pltpu.VMEM((2, RANGE, frames, KWIN), jnp.bfloat16),
            dma((3,)), dma((2,)), dma, dma, dma, dma, dma((CHUNKS,)), dma, dma((2, CHUNKS)), dma((CHUNKS // 2,)),
            pltpu.SemaphoreType.REGULAR((2,)),
            dma, dma((2, CHUNKS - DIRECT)),
        ],
        compiler_params=pltpu.CompilerParams(collective_id=0, has_side_effects=True),
    )(traces, tables, slab_range, table_slot, sample_start)


def solution(mesh):
    placed = (
        P(("slab", "det"), None, None),
        P("slab", None, "det"),
        P(("slab", "det"), None),
        P(("slab", "det"), None),
        P(("slab", "det"), None),
    )
    return jax.shard_map(
        functools.partial(body, mesh.shape["slab"]),
        mesh=mesh, in_specs=placed, out_specs=P(None, ("slab", "det")), check_vma=False,
    )
```
